256 devices in a mesh: groups: 4 (over x, y), ctx: 64 (over z, core).
Axes of the slice: x: 2, y: 2, z: 32, core: 2. Of those that a mesh axis runs over, the one named last changes fastest.
The devices are a block of a 4x8x32 slice.
Arguments:
- queries: bfloat16 [1024, 8192], P(('groups', 'ctx')), parts along dimension 0, may hold values from -200 to 200
- new_kv: bfloat16 [1024, 1024], P(('groups', 'ctx')), parts along dimension 0, may hold values from -9 to 9
- prefix_cache: bfloat16 [262144, 1024], P(('groups', 'ctx')), parts along dimension 0, may hold values from -6.5 to 6.5
- positions: int32 [1024], P('groups'), parts along dimension 0, may hold values from 0 to 255, each once
- lengths: int32 [256], P('groups'), parts along dimension 0, may hold values from 1 to 1024, 49152 in all
- out_weight: bfloat16 [8192, 16384], P(None, 'ctx'), may hold values from -0.0625 to 0.0625
Outputs:
- attended: bfloat16 [1024, 8192], P(('groups', 'ctx')), parts along dimension 0
- projected: bfloat16 [1024, 16384], P('groups', 'ctx'), parts along dimension 0
The draws below stay inside these ranges and needn't reach their ends.
There are 4 independent parts, one for each index of `groups`. The reference program is written for one: setup_inputs(seed, part) draws one part's arguments, and reference() takes and returns one part's arrays. A program takes and returns all parts, laid end to end along the dimension named above; an argument that names none is the same for every part. Nothing has to cross between parts.
Inputs may be any that keep to these rules, and one draw needn't show every extreme that they name: `positions`: a permutation of 0 to 255. The filled slots of shard i are its first lengths[i] slots; they sum to 49152, and some shard is full.
All inputs are finite; a program needn't handle non-finite values.
Results may differ from the reference program's by a relative error of at most 0.0045.
Values may be sent and summed in bfloat16 or wider, within the bound.
No kernel may reach another device: no remote copies, remote signals or barrier semaphores. Data moves between devices by JAX's collectives and lax.ppermute only.
A program may use at most 128 MiB of HBM per device.

```python
import math
import jax
import jax.numpy as jnp
import numpy as np
from jax import lax

D = 16384
HQ = 64
KVH = 4
HD = 128
BLK = 256
PCAP = 1024
TURN = 256
PREFIX = 49152
N_CTX = 64


def drawn(key):
    base_key = jax.random.fold_in(key, 7101)
    cache_key = jax.random.fold_in(key, 7102)
    scale_key = jax.random.fold_in(key, 7103)
    top_log = math.log(10.0)
    noise = jnp.clip(jax.random.normal(base_key, (TURN, HQ, HD), jnp.float32), -6.0, 6.0)
    head_scales = jnp.exp(jax.random.uniform(scale_key, (TURN, HQ, 1), jnp.float32, 0.0, top_log))
    query_rows = (2.5 * noise * head_scales).reshape(TURN, HQ * HD)
    cache_rows = jnp.clip(jax.random.normal(cache_key, (N_CTX * PCAP, KVH * 2 * HD), jnp.float32), -6.0, 6.0)
    return (query_rows, cache_rows)


def draw_queries(key, part):
    return drawn(key)[0].astype(jnp.bfloat16)


def draw_prefix_cache(key, part):
    return drawn(key)[1].astype(jnp.bfloat16)


def block_levels(key, dims, pieces, low, largest):
    def one(position, shards_of):
        draws = jax.random.uniform(jax.random.fold_in(jax.random.fold_in(key, 6), position), (shards_of,), jnp.float32, low / len(pieces), largest / len(pieces))
        return jnp.repeat(jnp.exp(draws), dims[position] // shards_of).reshape((-1,) + (1,) * (len(dims) - position - 1))

    level = one(*pieces[0])
    for cut in pieces[1:]:
        level = level * one(*cut)
    return level


def split_up(number_of, total, reach, skew):
    weights = [(1 << 20) // math.isqrt(grade ** skew) + 1 for grade in range(2, number_of + 1)]
    surplus, given = total - reach - (number_of - 1), [1] * (number_of - 1)
    while surplus > 0:
        free = [i for i in range(number_of - 1) if given[i] < reach]
        mass, left = sum([weights[i] for i in free]), surplus
        for i in free:
            addition = min(reach - given[i], max(1, left * weights[i] // mass), surplus)
            given[i] = given[i] + addition
            surplus = surplus - addition
    return np.array([reach] + given)


def uneven(stream_key, amount, total, bound, skew):
    if amount == 2:
        one = jax.random.randint(stream_key, (), max(1, total - bound), min(bound, total - 1) + 1)
        return jnp.stack([one, total - one])
    sizes = jnp.asarray(split_up(amount, total, bound, skew), jnp.int32)
    twos = (amount - 1) // 2
    giver, receiver = sizes[1:1 + 2 * twos:2], sizes[2:2 + 2 * twos:2]
    margin = jnp.minimum(giver - 1, bound - receiver)
    passed = jax.random.randint(jax.random.fold_in(stream_key, 1), (twos,), 0, 1 << 20) % (margin + 1)
    sizes = sizes.at[1:1 + 2 * twos:2].set(giver - passed).at[2:2 + 2 * twos:2].set(receiver + passed)
    return sizes[jax.random.permutation(jax.random.fold_in(stream_key, 2), amount)]


def bell_draw(rng, shape, spread, bound, cuts=(), kind=jnp.bfloat16):
    entries = jax.random.normal(rng, shape, jnp.float32) * spread
    if len(cuts) > 0:
        entries = block_levels(rng, shape, cuts, -0.22, 0.18) * entries
    return jnp.clip(entries, min=-bound, max=bound).astype(kind)


def setup_inputs(seed: int = 0, part: int = 0) -> dict:
    streams_of = jax.random.split(jax.random.key(seed), 7)
    part_splits = jax.random.split(jax.random.fold_in(streams_of[6], part), 7)
    return {
        "queries": draw_queries(jax.random.fold_in(jax.random.fold_in(streams_of[6], part), 71), part),
        "new_kv": bell_draw(part_splits[1], (TURN, KVH * 2 * HD), 1.5, 9.0, ((0, 64),)),
        "prefix_cache": draw_prefix_cache(jax.random.fold_in(jax.random.fold_in(streams_of[6], part), 71), part),
        "positions": jax.random.permutation(part_splits[3], TURN).astype(jnp.int32),
        "lengths": uneven(part_splits[4], N_CTX, PREFIX, PCAP, 2).astype(jnp.int32),
        "out_weight": bell_draw(streams_of[5], (HQ * HD, D), (HQ * HD) ** -0.5, 0.0625, ((1, 64),)),
    }


very_low = -1e+30

def block_stats(rows_q, key_rows, values, live_mask):
    scores = jnp.einsum('grd,gkd->grk', rows_q.astype(jnp.float32), key_rows.astype(jnp.float32)) * (1.0 / math.sqrt(HD))
    scores = jnp.where(live_mask, scores, very_low)
    row_max = lax.optimization_barrier(jnp.max(scores, axis=-1))
    weights = jnp.where(live_mask, jnp.exp(scores - row_max[..., None]), 0.0)
    row_total = lax.optimization_barrier(jnp.sum(weights, axis=-1))
    rounded = lax.optimization_barrier(weights.astype(jnp.bfloat16))
    summed = jnp.einsum('grk,gkd->grd', rounded.astype(jnp.float32), values.astype(jnp.float32))
    return (row_max, summed, row_total)

def fold_stats(running, fresh):
    old_max, old_sum, old_total = running
    new_max, new_sum, new_total = fresh
    joint_max = jnp.maximum(old_max, new_max)
    keep_old = jnp.exp(old_max - joint_max)
    keep_new = jnp.exp(new_max - joint_max)
    return (joint_max, old_sum * keep_old[..., None] + new_sum * keep_new[..., None], old_total * keep_old + new_total * keep_new)

def reference(queries, new_kv, prefix_cache, positions, lengths, out_weight):
    per_group = HQ // KVH
    all_rows = TURN * per_group
    group_rows = queries.reshape(TURN, KVH, per_group, HD).transpose(1, 0, 2, 3).reshape(KVH, all_rows, HD)
    block_count = N_CTX * PCAP // BLK
    blocks = prefix_cache.reshape(block_count, BLK, KVH, 2, HD)
    keys_all = blocks[:, :, :, 0].transpose(0, 2, 1, 3)
    values_all = blocks[:, :, :, 1].transpose(0, 2, 1, 3)
    slot_ids = jnp.arange(N_CTX * PCAP, dtype=jnp.int32)
    shard_of = slot_ids // PCAP
    live_all = (slot_ids % PCAP < lengths[shard_of]).reshape(block_count, BLK)
    start_state = (jnp.full((KVH, all_rows), very_low, jnp.float32), jnp.zeros((KVH, all_rows, HD), jnp.float32), jnp.zeros((KVH, all_rows), jnp.float32))

    def step(running, item):
        key_rows, values, live_row = item
        fresh = block_stats(group_rows, key_rows, values, live_row[None, None, :])
        return (fold_stats(running, fresh), None)
    running, _ = lax.scan(step, start_state, (keys_all, values_all, live_all))
    kv_view = new_kv.reshape(TURN, KVH, 2, HD)
    new_keys = kv_view[:, :, 0].transpose(1, 0, 2)
    new_values = kv_view[:, :, 1].transpose(1, 0, 2)
    causal = positions[:, None] >= positions[None, :]
    causal = jnp.repeat(causal, per_group, axis=0)
    fresh = block_stats(group_rows, new_keys, new_values, causal[None])
    combined = fold_stats(running, fresh)
    result = combined[1] / combined[2][..., None]
    attended = result.reshape(KVH, TURN, per_group, HD).transpose(1, 0, 2, 3).reshape(TURN, HQ * HD).astype(jnp.bfloat16)
    projected = jnp.dot(attended, out_weight, preferred_element_type=jnp.float32).astype(jnp.bfloat16)
    return (attended, projected)
```

```python
import functools
import math

import jax
import jax.numpy as jnp
from jax import lax
from jax.experimental import pallas as pl
from jax.experimental.pallas import tpu as pltpu
from jax.sharding import PartitionSpec as P

HQ = 64
KVH = 4
HD = 128
CTX = "ctx"
SPREAD = ("groups", "ctx")
PIECE = 512
TAIL = 16
ROWS = HD + TAIL
DEAD = -1e30
TO_LOG2 = math.log2(math.e) / math.sqrt(HD)


def prepare_body(lens_ref, mine_k, mine_v, theirs_k, theirs_v, keys_out, values_out):
    slots = mine_k.shape[0]
    lane = lax.broadcasted_iota(jnp.int32, (slots, HD), 1)
    row = lax.broadcasted_iota(jnp.int32, (slots, HD), 0)
    for half, (k_ref, v_ref) in enumerate(((mine_k, mine_v), (theirs_k, theirs_v))):
        dead = jnp.where((lane == 0) & (row >= lens_ref[half + 1]), DEAD, 0.0)
        span = pl.ds(half * slots, slots)
        keys_out[0, span, :HD] = k_ref[...]
        keys_out[0, span, HD:] = dead.astype(jnp.bfloat16)
        values_out[0, :, span] = v_ref[...].T


def prepare(core_lens, cache, theirs):
    slots = cache.shape[0]
    mine = lambda part: pl.BlockSpec((slots, HD), lambda g, s: (0, s[0] * KVH + 2 * g + part))
    other = lambda part: pl.BlockSpec((slots, HD), lambda g, s: (0, 2 * g + part))
    return pl.pallas_call(
        prepare_body,
        grid_spec=pltpu.PrefetchScalarGridSpec(
            num_scalar_prefetch=1,
            grid=(KVH // 2,),
            in_specs=[mine(0), mine(1), other(0), other(1)],
            out_specs=[
                pl.BlockSpec((1, 2 * slots, 2 * HD), lambda g, s: (g, 0, 0)),
                pl.BlockSpec((1, HD, 2 * slots), lambda g, s: (g, 0, 0)),
            ],
        ),
        out_shape=[
            jax.ShapeDtypeStruct((KVH // 2, 2 * slots, 2 * HD), jnp.bfloat16),
            jax.ShapeDtypeStruct((KVH // 2, HD, 2 * slots), jnp.bfloat16),
        ],
        name="prepare",
    )(core_lens, cache, cache, theirs, theirs)


def tail_rows(level):
    first = level.astype(jnp.bfloat16).astype(jnp.float32)
    second = (level - first).astype(jnp.bfloat16).astype(jnp.float32)
    third = level - first - second
    row = lax.broadcasted_iota(jnp.int32, (TAIL, level.shape[1]), 0)
    wide = jnp.where(row == 0, first, jnp.where(row == 1, second, jnp.where(row == 2, third, 0.0)))
    return wide.astype(jnp.bfloat16)


def level_of(tail):
    wide = tail.astype(jnp.float32)
    return wide[0:1] + wide[1:2] + wide[2:3]


def attend_body(pos_new, keys_ref, values_ref, new_k, new_v, *refs):
    count = len(refs) // 3
    slots = keys_ref.shape[1]
    for q_ref, pos_ref, out_ref in zip(refs[:count], refs[count : 2 * count], refs[2 * count :]):

        def tile(i, carry, q_ref=q_ref, pos_ref=pos_ref, out_ref=out_ref):
            q = jnp.concatenate([q_ref[2 * i, 0], q_ref[2 * i + 1, 0]], axis=0)
            at = jnp.concatenate([pos_ref[2 * i], pos_ref[2 * i + 1]], axis=1)
            lane = lax.broadcasted_iota(jnp.int32, q.shape, 1)
            q_wide = jnp.concatenate([q, jnp.where(lane == 0, 1.0, 0.0).astype(q.dtype)], axis=1)
            nt = (((1,), (1,)), ((), ()))
            found = []
            for first in range(0, slots, PIECE):
                span = slice(first, first + PIECE)
                s = lax.dot_general(keys_ref[0, span, :], q_wide, nt, preferred_element_type=jnp.float32)
                top = jnp.max(s, axis=0, keepdims=True)
                p = jnp.exp2((s - top) * TO_LOG2)
                total = jnp.sum(p, axis=0, keepdims=True)
                summed = jnp.dot(
                    values_ref[0, :, span], p.astype(jnp.bfloat16), preferred_element_type=jnp.float32
                )
                found.append((top, total, summed))
            s = lax.dot_general(new_k[0], q, nt, preferred_element_type=jnp.float32)
            s = jnp.where(at >= pos_new[...], s, DEAD)
            top = jnp.max(s, axis=0, keepdims=True)
            p = jnp.exp2((s - top) * TO_LOG2)
            total = jnp.sum(p, axis=0, keepdims=True)
            summed = lax.dot_general(
                new_v[0], p.astype(jnp.bfloat16), (((0,), (0,)), ((), ())), preferred_element_type=jnp.float32
            )
            found.append((top, total, summed))
            best = functools.reduce(jnp.maximum, [f[0] for f in found])
            weights = [jnp.exp2((f[0] - best) * TO_LOG2) for f in found]
            total = sum(w * f[1] for w, f in zip(weights, found))
            out = sum(w * f[2] for w, f in zip(weights, found)) * (1.0 / total)
            out = out.astype(jnp.bfloat16)
            tail = tail_rows(best * TO_LOG2 + jnp.log2(total))
            for k in range(2):
                lanes = slice(k * HD, (k + 1) * HD)
                out_ref[2 * i + k, 0, :HD, :] = out[:, lanes]
                out_ref[2 * i + k, 0, HD:, :] = tail[:, lanes]
            return carry

        lax.fori_loop(0, q_ref.shape[0] // 2, tile, 0)


def attend(prepared, pos_new, new_k, new_v, blocks, places):
    keys, values = prepared
    per_group = lambda a: pl.BlockSpec((1, *a.shape[1:]), lambda g: (g, 0, 0))
    whole = lambda a: pl.BlockSpec(a.shape, lambda g: (0,) * a.ndim)
    one = lambda a, rows: pl.BlockSpec((a.shape[0], 1, rows, HD), lambda g: (0, g, 0, 0))
    return pl.pallas_call(
        attend_body,
        grid=(KVH // 2,),
        in_specs=[whole(pos_new), per_group(keys), per_group(values), per_group(new_k), per_group(new_v)]
        + [one(b, HD) for b in blocks]
        + [whole(p) for p in places],
        out_specs=[one(b, ROWS) for b in blocks],
        out_shape=[jax.ShapeDtypeStruct((b.shape[0], KVH // 2, ROWS, HD), jnp.bfloat16) for b in blocks],
        compiler_params=pltpu.CompilerParams(vmem_limit_bytes=48 * 1024 * 1024),
        name="attend",
    )(pos_new, keys, values, new_k, new_v, *blocks, *places)


def merged(parts):
    levels = [level_of(t) for _, t in parts]
    best = functools.reduce(jnp.maximum, levels)
    weights = [jnp.exp2(v - best) for v in levels]
    total = sum(weights)
    out = sum(w * o.astype(jnp.float32) for w, (o, _) in zip(weights, parts)) * (1.0 / total)
    return out, best + jnp.log2(total)


def merge_body(starts, *refs):
    out_ref = refs[-1]
    for b in range(out_ref.shape[0]):
        inside = [
            (r, b - k) for r, k in zip(refs[:-1], starts) if 0 <= b - k < r.shape[0]
        ]
        for g in range(out_ref.shape[1]):
            if len(inside) == 1:
                out_ref[b, g] = inside[0][0][b, g]
                continue
            out, level = merged([(r[i, g, :HD, :], r[i, g, HD:, :]) for r, i in inside])
            out_ref[b, g, :HD, :] = out.astype(jnp.bfloat16)
            out_ref[b, g, HD:, :] = tail_rows(level)


def merge(mine, *others):
    arrays = (mine,) + tuple(a for a, _ in others)
    starts = (0,) + tuple(k for _, k in others)
    return pl.pallas_call(
        functools.partial(merge_body, starts),
        out_shape=jax.ShapeDtypeStruct(mine.shape, mine.dtype),
        name="merge",
    )(*arrays)


def finish_body(*refs):
    out_ref = refs[-1]
    for g in range(out_ref.shape[0]):
        out, _ = merged([(r[0, g, :HD, :], r[0, g, HD:, :]) for r in refs[:-1]])
        out_ref[g] = out.T.astype(jnp.bfloat16)


def finish(*arrays):
    return pl.pallas_call(
        finish_body,
        out_shape=jax.ShapeDtypeStruct((KVH // 2, HD, HD), jnp.bfloat16),
        name="finish",
    )(*arrays)


def shards(queries, new_kv, prefix_cache, positions, lengths, out_weight):
    devices = lax.axis_size(CTX)
    chips = devices // 2
    far = chips // 4
    reach = far // 2
    index = lax.axis_index(CTX)
    chip, core = index // 2, index % 2
    tokens = queries.shape[0]
    per_group = HQ // KVH
    half = HQ * HD // 2

    def take(x, d):
        return lax.ppermute(x, CTX, [(i, (i - 2 * d) % devices) for i in range(devices)])

    def swap(x):
        return lax.ppermute(x, CTX, [(i, i ^ 1) for i in range(devices)])

    def halves(x, axis):
        width = x.shape[axis] // 2
        keep = lax.dynamic_slice_in_dim(x, core * width, width, axis)
        send = lax.dynamic_slice_in_dim(x, (1 - core) * width, width, axis)
        return keep, send

    def in_order(mine, theirs):
        return jnp.where(core == 0, jnp.concatenate([mine, theirs]), jnp.concatenate([theirs, mine]))

    def gathered(block):
        block = block[None]
        ring = jnp.concatenate([take(block, -far), block, take(block, far), take(block, 2 * far)])
        chunks = {0: ring}
        right = left = ring
        for s in range(1, reach):
            right, left = take(right, 1), take(left, -1)
            chunks[s], chunks[-s] = right, left
        chunks[reach], chunks[-reach] = take(right[1:3], 1), take(left[0:2], -1)
        return chunks

    def offsets(s):
        if s == reach:
            return [s, s + far]
        if s == -reach:
            return [(s - far) % chips, s % chips]
        return [(s + k * far) % chips for k in (-1, 0, 1, 2)]

    q_mine, q_send = halves(queries, 1)
    n_mine, n_send = halves(new_kv, 1)
    small = swap(jnp.concatenate([q_send, n_send], axis=1))
    q_block = in_order(q_mine, small[:, :half])
    q_block = q_block.reshape(2 * tokens, KVH // 2, per_group, HD).transpose(1, 0, 2, 3)
    q_block = q_block.reshape(KVH // 2, 2 * tokens * per_group, HD)
    new_rows = jnp.concatenate([n_mine, small[:, half:]])
    new_rows = jnp.pad(new_rows, ((0, TAIL - 2 * tokens), (0, 0))).reshape(TAIL, KVH // 2, 2, HD)
    new_k, new_v = new_rows[:, :, 0].transpose(1, 0, 2), new_rows[:, :, 1].transpose(1, 0, 2)
    pos_of = lambda who: lax.dynamic_slice_in_dim(positions, who * tokens, tokens, 0)
    pos_new = jnp.concatenate([pos_of(index), pos_of(index ^ 1)])
    pos_new = jnp.pad(pos_new, (0, TAIL - 2 * tokens), constant_values=positions.shape[0])[:, None]
    placed = jnp.repeat(positions.reshape(chips, 2 * tokens), per_group, axis=1)
    placed = lax.dynamic_slice_in_dim(jnp.concatenate([placed, placed]), chip, chips, 0)
    placed = placed[:, None, :]

    q_chunks = gathered(q_block)
    width = prefix_cache.shape[1] // 2
    theirs = swap(lax.dynamic_slice_in_dim(prefix_cache, (1 - core) * width, width, 1))
    length_of = lambda who: lax.dynamic_index_in_dim(lengths, who, 0, keepdims=False)
    core_lens = jnp.stack([core, length_of(index), length_of(index ^ 1)]).astype(jnp.int32)
    prepared = prepare(core_lens, prefix_cache, theirs)
    w_mine, w_send = halves(out_weight, 0)
    w_theirs = swap(w_send)

    parts = {}
    for group in [(0,)] + [(s, -s) for s in range(1, reach + 1)]:
        places = [jnp.stack([placed[o] for o in offsets(s)]) for s in group]
        outs = attend(prepared, pos_new, new_k, new_v, [q_chunks[s] for s in group], places)
        parts.update(zip(group, outs))

    right, left = take(parts[reach], -1), take(parts[-reach], 1)
    for s in range(reach - 1, 0, -1):
        starts = (1, 0) if s == reach - 1 else (0, 0)
        right = take(merge(parts[s], (right, starts[0])), -1)
        left = take(merge(parts[-s], (left, starts[1])), 1)
    ring = merge(parts[0], (right, 0), (left, 0))
    own = finish(
        ring[1:2], take(ring[2:3], -far), take(ring[0:1], far), take(ring[3:4], 2 * far)
    )
    rows = own.reshape(KVH // 2, 2 * tokens, per_group, HD).transpose(1, 0, 2, 3).reshape(2 * tokens, half)

    keep = lax.dynamic_slice_in_dim(rows, core * tokens, tokens, 0)
    other = swap(lax.dynamic_slice_in_dim(rows, (1 - core) * tokens, tokens, 0))
    attended = jnp.where(
        core == 0, jnp.concatenate([keep, other], axis=1), jnp.concatenate([other, keep], axis=1)
    )

    row_chunks = gathered(rows)
    spans = [range(1 - reach, reach), (reach, -reach)]
    mine, theirs = [], []
    order = []
    for span in spans:
        lhs = jnp.concatenate([row_chunks[s] for s in span]).reshape(-1, half)
        order += [o for s in span for o in offsets(s)]
        theirs.append(jnp.dot(lhs, w_theirs, preferred_element_type=jnp.float32))
        mine.append(jnp.dot(lhs, w_mine, preferred_element_type=jnp.float32))
    out = jnp.concatenate(mine) + swap(jnp.concatenate(theirs))
    out = out.astype(jnp.bfloat16).reshape(chips, 2 * tokens, -1)
    out = jnp.stack([out[order.index(o)] for o in range(chips)])
    out = lax.dynamic_slice_in_dim(jnp.concatenate([out, out]), chips - chip, chips, 0)
    return attended, out.reshape(chips * 2 * tokens, -1)


def solution(mesh):
    return jax.shard_map(
        shards,
        mesh=mesh,
        in_specs=(
            P(SPREAD, None),
            P(SPREAD, None),
            P(SPREAD, None),
            P("groups"),
            P("groups"),
            P(None, CTX),
        ),
        out_specs=(P(SPREAD, None), P("groups", CTX)),
        check_vma=False,
    )
```

```python
import functools
import math

import jax
import jax.numpy as jnp
from jax import lax
from jax.experimental import pallas as pl
from jax.experimental.pallas import tpu as pltpu
from jax.sharding import PartitionSpec as P

HQ = 64
KVH = 4
HD = 128
CTX = "ctx"
SPREAD = ("groups", "ctx")
TILE = 4
HOP = 4
TAIL = 16
ROWS = HD + TAIL
DEAD = -1e30
TO_LOG2 = math.log2(math.e) / math.sqrt(HD)


def prepare_body(lens_ref, mine_k, mine_v, theirs_k, theirs_v, keys_out, values_out):
    slots = mine_k.shape[0]
    lane = lax.broadcasted_iota(jnp.int32, (slots, HD), 1)
    row = lax.broadcasted_iota(jnp.int32, (slots, HD), 0)
    for half, (k_ref, v_ref) in enumerate(((mine_k, mine_v), (theirs_k, theirs_v))):
        dead = jnp.where((lane == 0) & (row >= lens_ref[half + 1]), DEAD, 0.0)
        span = pl.ds(half * slots, slots)
        keys_out[0, span, :HD] = k_ref[...]
        keys_out[0, span, HD:] = dead.astype(jnp.bfloat16)
        values_out[0, :, span] = v_ref[...].T


def prepare(core_lens, cache, theirs):
    slots = cache.shape[0]
    mine = lambda part: pl.BlockSpec((slots, HD), lambda g, s: (0, s[0] * KVH + 2 * g + part))
    return pl.pallas_call(
        prepare_body,
        grid_spec=pltpu.PrefetchScalarGridSpec(
            num_scalar_prefetch=1,
            grid=(KVH // 2,),
            in_specs=[mine(0), mine(1), mine(0), mine(1)],
            out_specs=[
                pl.BlockSpec((1, 2 * slots, 2 * HD), lambda g, s: (g, 0, 0)),
                pl.BlockSpec((1, HD, 2 * slots), lambda g, s: (g, 0, 0)),
            ],
        ),
        out_shape=[
            jax.ShapeDtypeStruct((KVH // 2, 2 * slots, 2 * HD), jnp.bfloat16),
            jax.ShapeDtypeStruct((KVH // 2, HD, 2 * slots), jnp.bfloat16),
        ],
        cost_estimate=pl.CostEstimate(flops=slots * HD * 2048, transcendentals=0, bytes_accessed=10 * slots * HD * KVH),
        name="prepare",
    )(core_lens, cache, cache, theirs, theirs)


def tail_rows(level):
    first = level.astype(jnp.bfloat16).astype(jnp.float32)
    second = (level - first).astype(jnp.bfloat16).astype(jnp.float32)
    third = level - first - second
    row = lax.broadcasted_iota(jnp.int32, (TAIL, level.shape[1]), 0)
    wide = jnp.where(row == 0, first, jnp.where(row == 1, second, jnp.where(row == 2, third, 0.0)))
    return wide.astype(jnp.bfloat16)


def level_of(tail):
    wide = tail.astype(jnp.float32)
    return wide[0:1] + wide[1:2] + wide[2:3]


def attend_body(pos_new, keys_ref, values_ref, new_k, new_v, *refs):
    count = len(refs) // 3
    nt = (((1,), (1,)), ((), ()))
    tn = (((0,), (0,)), ((), ()))

    def softmax(s):
        top = jnp.max(s, axis=0, keepdims=True)
        p = jnp.exp2((s - top) * TO_LOG2)
        return top, jnp.sum(p, axis=0, keepdims=True), p.astype(jnp.bfloat16)

    for q_ref, pos_ref, out_ref in zip(refs[:count], refs[count : 2 * count], refs[2 * count :]):

        def tile(i, carry, q_ref=q_ref, pos_ref=pos_ref, out_ref=out_ref):
            base = i * TILE
            q = jnp.concatenate([q_ref[base + k, 0] for k in range(TILE)], axis=0)
            at = jnp.concatenate([pos_ref[base + k] for k in range(TILE)], axis=1)
            lane = lax.broadcasted_iota(jnp.int32, q.shape, 1)
            q_wide = jnp.concatenate([q, jnp.where(lane == 0, 1.0, 0.0).astype(q.dtype)], axis=1)
            s = lax.dot_general(keys_ref[0], q_wide, nt, preferred_element_type=jnp.float32)
            top_a, total_a, p = softmax(s)
            out_a = jnp.dot(values_ref[0], p, preferred_element_type=jnp.float32)
            s = lax.dot_general(new_k[0], q, nt, preferred_element_type=jnp.float32)
            top_b, total_b, p = softmax(jnp.where(at >= pos_new[...], s, DEAD))
            out_b = lax.dot_general(new_v[0], p, tn, preferred_element_type=jnp.float32)
            best = jnp.maximum(top_a, top_b)
            keep_a = jnp.exp2((top_a - best) * TO_LOG2)
            keep_b = jnp.exp2((top_b - best) * TO_LOG2)
            total = keep_a * total_a + keep_b * total_b
            out = (keep_a * out_a + keep_b * out_b) * (1.0 / total)
            out = out.astype(jnp.bfloat16)
            tail = tail_rows(best * TO_LOG2 + jnp.log2(total))
            for k in range(TILE):
                lanes = slice(k * HD, (k + 1) * HD)
                out_ref[base + k, 0, :HD, :] = out[:, lanes]
                out_ref[base + k, 0, HD:, :] = tail[:, lanes]
            return carry

        if q_ref.shape[0] == TILE:
            tile(0, 0)
        else:
            lax.fori_loop(0, q_ref.shape[0] // TILE, tile, 0)


def attend(prepared, pos_new, new_k, new_v, blocks, places):
    keys, values = prepared
    per_group = lambda a: pl.BlockSpec((1, *a.shape[1:]), lambda g: (g, 0, 0))
    whole = lambda a: pl.BlockSpec(a.shape, lambda g: (0,) * a.ndim)
    one = lambda a, rows: pl.BlockSpec((a.shape[0], 1, rows, HD), lambda g: (0, g, 0, 0))
    score_count = sum(b.shape[0] for b in blocks) * HD * keys.shape[0] * keys.shape[1]
    return pl.pallas_call(
        attend_body,
        grid=(KVH // 2,),
        in_specs=[whole(pos_new), per_group(keys), per_group(values), per_group(new_k), per_group(new_v)]
        + [one(b, HD) for b in blocks]
        + [whole(p) for p in places],
        out_specs=[one(b, ROWS) for b in blocks],
        out_shape=[jax.ShapeDtypeStruct((b.shape[0], KVH // 2, ROWS, HD), jnp.bfloat16) for b in blocks],
        compiler_params=pltpu.CompilerParams(vmem_limit_bytes=48 * 1024 * 1024),
        cost_estimate=pl.CostEstimate(
            flops=score_count * 6 * HD,
            transcendentals=score_count,
            bytes_accessed=2 * (keys.size + values.size + 2 * sum(b.size for b in blocks)),
        ),
        name="attend",
    )(pos_new, keys, values, new_k, new_v, *blocks, *places)


def merged(parts):
    levels = [level_of(t) for _, t in parts]
    best = functools.reduce(jnp.maximum, levels)
    weights = [jnp.exp2(v - best) for v in levels]
    total = sum(weights)
    out = sum(w * o.astype(jnp.float32) for w, (o, _) in zip(weights, parts)) * (1.0 / total)
    return out, best + jnp.log2(total)


def merge_body(jobs, *refs):
    ins, outs = list(refs[: -len(jobs)]), refs[-len(jobs) :]
    for starts, out_ref in zip(jobs, outs):
        parts = [(ins.pop(0), b0, g0) for b0, g0 in starts]
        for g in range(out_ref.shape[1]):
            here = [(r, b0, g - g0) for r, b0, g0 in parts if 0 <= g - g0 < r.shape[1]]
            cuts = sorted({c for r, b0, _ in here for c in (b0, b0 + r.shape[0])})
            for low, high in zip(cuts[:-1], cuts[1:]):
                live = [(r, b0, k) for r, b0, k in here if b0 <= low and high <= b0 + r.shape[0]]

                def visit(b, carry, live=live, g=g, out_ref=out_ref):
                    if len(live) == 1:
                        r, b0, k = live[0]
                        out_ref[b, g] = r[b - b0, k]
                        return carry
                    out, level = merged(
                        [(r[b - b0, k, :HD, :], r[b - b0, k, HD:, :]) for r, b0, k in live]
                    )
                    out_ref[b, g, :HD, :] = out.astype(jnp.bfloat16)
                    out_ref[b, g, HD:, :] = tail_rows(level)
                    return carry

                if high - low == 1:
                    visit(low, 0)
                else:
                    lax.fori_loop(low, high, visit, 0)


def merge(*jobs):
    arrays = [a for job in jobs for a, _, _ in job]
    starts = tuple(tuple((b0, g0) for _, b0, g0 in job) for job in jobs)
    return pl.pallas_call(
        functools.partial(merge_body, starts),
        out_shape=[jax.ShapeDtypeStruct(job[0][0].shape, job[0][0].dtype) for job in jobs],
        name="merge",
    )(*arrays)


def finish_body(*refs):
    out_ref = refs[-1]
    for g in range(out_ref.shape[0]):
        out, _ = merged([(r[0, g, :HD, :], r[0, g, HD:, :]) for r in refs[:-1]])
        out_ref[g] = out.T.astype(jnp.bfloat16)


def finish(*arrays):
    return pl.pallas_call(
        finish_body,
        out_shape=jax.ShapeDtypeStruct((KVH // 2, HD, HD), jnp.bfloat16),
        name="finish",
    )(*arrays)


def shards(queries, new_kv, prefix_cache, positions, lengths, out_weight):
    devices = lax.axis_size(CTX)
    chips = devices // 2
    ring = chips // HOP
    low = ring // 2 - 1
    index = lax.axis_index(CTX)
    chip, core = index // 2, index % 2
    tokens = queries.shape[0]
    per_group = HQ // KVH
    half = HQ * HD // 2

    def take(x, d):
        return lax.ppermute(x, CTX, [(i, (i - 2 * d) % devices) for i in range(devices)])

    def swap(x):
        return lax.ppermute(x, CTX, [(i, i ^ 1) for i in range(devices)])

    def halves(x, axis):
        width = x.shape[axis] // 2
        keep = lax.dynamic_slice_in_dim(x, core * width, width, axis)
        send = lax.dynamic_slice_in_dim(x, (1 - core) * width, width, axis)
        return keep, send

    def in_order(mine, theirs):
        return jnp.where(core == 0, jnp.concatenate([mine, theirs]), jnp.concatenate([theirs, mine]))

    def after(first, *then):
        return lax.optimization_barrier((*then, first))[:-1]

    def gathered(block, axis, side=(), last=lambda own: ()):
        width = block.shape[axis] // 2
        up = down = block[None]
        found = [up]
        for _ in range(low):
            up, down = take(up, HOP), take(down, -HOP)
            found = [down] + found + [up]
            if side:
                up, down = after(side[0], up, down)
                side = side[1:]
        first = lax.slice_in_dim(up, 0, width, axis=axis + 1)
        second = lax.slice_in_dim(down, width, 2 * width, axis=axis + 1)
        found.append(jnp.concatenate([take(first, HOP), take(second, -HOP)], axis=axis + 1))
        own = jnp.concatenate(found)
        right, left = take(own, 1), take(own, -1)
        done = last(own)
        right, left = after(done, right, left)
        return own, right, left, take(right[low : low + ring // 2], 1), take(left[: ring // 2], -1), done

    stretch = [HOP * k for k in range(-low, ring - low)]
    near = [
        [k + s for k in stretch] for s in (0, 1, -1)
    ] + [[k + 2 for k in stretch[low : low + ring // 2]], [k - 2 for k in stretch[: ring // 2]]]

    q_mine, q_send = halves(queries, 1)
    n_mine, n_send = halves(new_kv, 1)
    small = swap(jnp.concatenate([q_send, n_send], axis=1))
    theirs = swap(prefix_cache)
    q_block = in_order(q_mine, small[:, :half])
    q_block = q_block.reshape(2 * tokens, KVH // 2, per_group, HD).transpose(1, 0, 2, 3)
    q_block = q_block.reshape(KVH // 2, 2 * tokens * per_group, HD)
    new_rows = jnp.concatenate([n_mine, small[:, half:]])
    new_rows = jnp.pad(new_rows, ((0, TAIL - 2 * tokens), (0, 0))).reshape(TAIL, KVH // 2, 2, HD)
    new_k, new_v = new_rows[:, :, 0].transpose(1, 0, 2), new_rows[:, :, 1].transpose(1, 0, 2)
    pos_of = lambda who: lax.dynamic_slice_in_dim(positions, who * tokens, tokens, 0)
    pos_new = jnp.concatenate([pos_of(index), pos_of(index ^ 1)])
    pos_new = jnp.pad(pos_new, (0, TAIL - 2 * tokens), constant_values=positions.shape[0])[:, None]
    placed = jnp.repeat(positions.reshape(chips, 2 * tokens), per_group, axis=1)
    placed = lax.dynamic_slice_in_dim(jnp.concatenate([placed, placed]), chip, chips, 0)
    placed = placed[:, None, :]
    length_of = lambda who: lax.dynamic_index_in_dim(lengths, who, 0, keepdims=False)
    core_lens = jnp.stack([core, length_of(index), length_of(index ^ 1)]).astype(jnp.int32)
    prepared = prepare(core_lens, prefix_cache, theirs)
    w_mine = lax.dynamic_slice_in_dim(out_weight, core * half, half, 0)

    w_send = lax.dynamic_slice_in_dim(out_weight, (1 - core) * half, half, 0)
    w_theirs = swap(w_send)
    places = [jnp.stack([placed[o % chips] for o in offsets]) for offsets in near]

    def score(blocks, *which):
        return attend(prepared, pos_new, new_k, new_v, blocks, [places[k] for k in which])

    own, right, left, right_far, left_far, parts_own = gathered(
        q_block, 0, (prepared, w_send), lambda own: score([own], 0)
    )
    parts_right = score([right], 1)
    right_far, left_far = after(parts_right, right_far, left_far)
    right_far, left_far = score([right_far, left_far], 3, 4)
    parts_left = score([left], 2)
    parts = [parts_own[0], parts_right[0], parts_left[0]]

    right, left = take(right_far, -1), take(left_far, 1)
    right, left = merge([(parts[1], 0, 0), (right, low, 0)], [(parts[2], 0, 0), (left, 0, 0)])
    right, left = after(w_theirs, right, left)
    right, left = take(right, -1), take(left, 1)
    (summed,) = merge([(parts[0], 0, 0), (right, 0, 0), (left, 0, 0)])
    up, down = take(summed[ring - 1 :, :1], -HOP), take(summed[ring - 1 :, 1:], HOP)
    for k in range(low, 0, -1):
        starts = (0, 1) if k == low else (0, 0)
        up, down = merge(
            [(summed[low + k : low + k + 1], 0, 0), (up, 0, starts[0])],
            [(summed[low - k : low - k + 1], 0, 0), (down, 0, starts[1])],
        )
        up, down = take(up, -HOP), take(down, HOP)
    own = finish(summed[low : low + 1], up, down)
    rows = own.reshape(KVH // 2, 2 * tokens, per_group, HD).transpose(1, 0, 2, 3).reshape(2 * tokens, half)

    keep = lax.dynamic_slice_in_dim(rows, core * tokens, tokens, 0)
    other = swap(lax.dynamic_slice_in_dim(rows, (1 - core) * tokens, tokens, 0))
    attended = jnp.where(
        core == 0, jnp.concatenate([keep, other], axis=1), jnp.concatenate([other, keep], axis=1)
    )

    own, right, left, right_far, left_far, _ = gathered(rows, 1)
    last = jnp.concatenate([left_far[1:], right_far, left_far[:1]])
    mine, other = [], []
    for lhs in (jnp.concatenate([left, own, right]), last):
        lhs = lhs.reshape(-1, half)
        other.append(jnp.dot(lhs, w_theirs, preferred_element_type=jnp.float32))
        mine.append(jnp.dot(lhs, w_mine, preferred_element_type=jnp.float32))
    out = jnp.concatenate(mine) + swap(jnp.concatenate(other))
    out = out.astype(jnp.bfloat16).reshape(HOP, ring, 2 * tokens, -1).transpose(1, 0, 2, 3)
    out = out.reshape(chips, 2 * tokens, -1)
    first = (HOP * low + 1 - chip) % chips
    out = lax.dynamic_slice_in_dim(jnp.concatenate([out, out]), first, chips, 0)
    return attended, out.reshape(chips * 2 * tokens, -1)


def solution(mesh):
    return jax.shard_map(
        shards,
        mesh=mesh,
        in_specs=(
            P(SPREAD, None),
            P(SPREAD, None),
            P(SPREAD, None),
            P("groups"),
            P("groups"),
            P(None, CTX),
        ),
        out_specs=(P(SPREAD, None), P("groups", CTX)),
        check_vma=False,
    )
```

```python
import functools
import math

import jax
import jax.numpy as jnp
from jax import lax
from jax.experimental import pallas as pl
from jax.experimental.pallas import tpu as pltpu
from jax.sharding import PartitionSpec as P

HQ = 64
KVH = 4
HD = 128
CTX = "ctx"
SPREAD = ("groups", "ctx")
TILE = 4
HOP = 4
TAIL = 16
ROWS = HD + TAIL
DEAD = -1e30
TO_LOG2 = math.log2(math.e) / math.sqrt(HD)


def prepare_body(lens_ref, mine_k, mine_v, theirs_k, theirs_v, keys_out, values_out):
    slots = mine_k.shape[0]
    lane = lax.broadcasted_iota(jnp.int32, (slots, HD), 1)
    row = lax.broadcasted_iota(jnp.int32, (slots, HD), 0)
    for half, (k_ref, v_ref) in enumerate(((mine_k, mine_v), (theirs_k, theirs_v))):
        dead = jnp.where((lane == 0) & (row >= lens_ref[half + 1]), DEAD, 0.0)
        span = pl.ds(half * slots, slots)
        keys_out[0, span, :HD] = k_ref[...]
        keys_out[0, span, HD:] = dead.astype(jnp.bfloat16)
        values_out[0, :, span] = v_ref[...].T


def prepare(core_lens, cache, theirs):
    slots = cache.shape[0]
    mine = lambda part: pl.BlockSpec((slots, HD), lambda g, s: (0, s[0] * KVH + 2 * g + part))
    return pl.pallas_call(
        prepare_body,
        grid_spec=pltpu.PrefetchScalarGridSpec(
            num_scalar_prefetch=1,
            grid=(KVH // 2,),
            in_specs=[mine(0), mine(1), mine(0), mine(1)],
            out_specs=[
                pl.BlockSpec((1, 2 * slots, 2 * HD), lambda g, s: (g, 0, 0)),
                pl.BlockSpec((1, HD, 2 * slots), lambda g, s: (g, 0, 0)),
            ],
        ),
        out_shape=[
            jax.ShapeDtypeStruct((KVH // 2, 2 * slots, 2 * HD), jnp.bfloat16),
            jax.ShapeDtypeStruct((KVH // 2, HD, 2 * slots), jnp.bfloat16),
        ],
        cost_estimate=pl.CostEstimate(flops=slots * HD * 2048, transcendentals=0, bytes_accessed=10 * slots * HD * KVH),
        name="prepare",
    )(core_lens, cache, cache, theirs, theirs)


def tail_rows(level):
    first = level.astype(jnp.bfloat16).astype(jnp.float32)
    second = (level - first).astype(jnp.bfloat16).astype(jnp.float32)
    third = level - first - second
    row = lax.broadcasted_iota(jnp.int32, (TAIL, level.shape[1]), 0)
    wide = jnp.where(row == 0, first, jnp.where(row == 1, second, jnp.where(row == 2, third, 0.0)))
    return wide.astype(jnp.bfloat16)


def level_of(tail):
    wide = tail.astype(jnp.float32)
    return wide[0:1] + wide[1:2] + wide[2:3]


def attend_body(pos_new, keys_ref, values_ref, new_k, new_v, *refs):
    count = len(refs) // 3
    nt = (((1,), (1,)), ((), ()))
    tn = (((0,), (0,)), ((), ()))

    def softmax(s):
        top = jnp.max(s, axis=0, keepdims=True)
        p = jnp.exp2((s - top) * TO_LOG2)
        return top, jnp.sum(p, axis=0, keepdims=True), p.astype(jnp.bfloat16)

    for q_ref, pos_ref, out_ref in zip(refs[:count], refs[count : 2 * count], refs[2 * count :]):

        def tile(i, carry, q_ref=q_ref, pos_ref=pos_ref, out_ref=out_ref):
            base = i * TILE
            q = jnp.concatenate([q_ref[base + k, 0] for k in range(TILE)], axis=0)
            at = jnp.concatenate([pos_ref[base + k] for k in range(TILE)], axis=1)
            lane = lax.broadcasted_iota(jnp.int32, q.shape, 1)
            q_wide = jnp.concatenate([q, jnp.where(lane == 0, 1.0, 0.0).astype(q.dtype)], axis=1)
            s = lax.dot_general(keys_ref[0], q_wide, nt, preferred_element_type=jnp.float32)
            top_a, total_a, p = softmax(s)
            out_a = jnp.dot(values_ref[0], p, preferred_element_type=jnp.float32)
            s = lax.dot_general(new_k[0], q, nt, preferred_element_type=jnp.float32)
            top_b, total_b, p = softmax(jnp.where(at >= pos_new[...], s, DEAD))
            out_b = lax.dot_general(new_v[0], p, tn, preferred_element_type=jnp.float32)
            best = jnp.maximum(top_a, top_b)
            keep_a = jnp.exp2((top_a - best) * TO_LOG2)
            keep_b = jnp.exp2((top_b - best) * TO_LOG2)
            total = keep_a * total_a + keep_b * total_b
            out = (keep_a * out_a + keep_b * out_b) * (1.0 / total)
            out = out.astype(jnp.bfloat16)
            tail = tail_rows(best * TO_LOG2 + jnp.log2(total))
            for k in range(TILE):
                lanes = slice(k * HD, (k + 1) * HD)
                out_ref[base + k, 0, :HD, :] = out[:, lanes]
                out_ref[base + k, 0, HD:, :] = tail[:, lanes]
            return carry

        if q_ref.shape[0] == TILE:
            tile(0, 0)
        else:
            lax.fori_loop(0, q_ref.shape[0] // TILE, tile, 0)


def attend(prepared, pos_new, new_k, new_v, blocks, places):
    keys, values = prepared
    per_group = lambda a: pl.BlockSpec((1, *a.shape[1:]), lambda g: (g, 0, 0))
    whole = lambda a: pl.BlockSpec(a.shape, lambda g: (0,) * a.ndim)
    one = lambda a, rows: pl.BlockSpec((a.shape[0], 1, rows, HD), lambda g: (0, g, 0, 0))
    score_count = sum(b.shape[0] for b in blocks) * HD * keys.shape[0] * keys.shape[1]
    return pl.pallas_call(
        attend_body,
        grid=(KVH // 2,),
        in_specs=[whole(pos_new), per_group(keys), per_group(values), per_group(new_k), per_group(new_v)]
        + [one(b, HD) for b in blocks]
        + [whole(p) for p in places],
        out_specs=[one(b, ROWS) for b in blocks],
        out_shape=[jax.ShapeDtypeStruct((b.shape[0], KVH // 2, ROWS, HD), jnp.bfloat16) for b in blocks],
        compiler_params=pltpu.CompilerParams(vmem_limit_bytes=48 * 1024 * 1024),
        cost_estimate=pl.CostEstimate(
            flops=score_count * 6 * HD,
            transcendentals=score_count,
            bytes_accessed=2 * (keys.size + values.size + 2 * sum(b.size for b in blocks)),
        ),
        name="attend",
    )(pos_new, keys, values, new_k, new_v, *blocks, *places)


def merged(parts):
    levels = [level_of(t) for _, t in parts]
    best = functools.reduce(jnp.maximum, levels)
    weights = [jnp.exp2(v - best) for v in levels]
    total = sum(weights)
    out = sum(w * o.astype(jnp.float32) for w, (o, _) in zip(weights, parts)) * (1.0 / total)
    return out, best + jnp.log2(total)


def merge_body(jobs, *refs):
    ins, outs = list(refs[: -len(jobs)]), refs[-len(jobs) :]
    for starts, out_ref in zip(jobs, outs):
        parts = [(ins.pop(0), b0, g0) for b0, g0 in starts]
        for g in range(out_ref.shape[1]):
            here = [(r, b0, g - g0) for r, b0, g0 in parts if 0 <= g - g0 < r.shape[1]]
            cuts = sorted({c for r, b0, _ in here for c in (b0, b0 + r.shape[0])})
            for low, high in zip(cuts[:-1], cuts[1:]):
                live = [(r, b0, k) for r, b0, k in here if b0 <= low and high <= b0 + r.shape[0]]

                def visit(b, carry, live=live, g=g, out_ref=out_ref):
                    if len(live) == 1:
                        r, b0, k = live[0]
                        out_ref[b, g] = r[b - b0, k]
                        return carry
                    out, level = merged(
                        [(r[b - b0, k, :HD, :], r[b - b0, k, HD:, :]) for r, b0, k in live]
                    )
                    out_ref[b, g, :HD, :] = out.astype(jnp.bfloat16)
                    out_ref[b, g, HD:, :] = tail_rows(level)
                    return carry

                if high - low == 1:
                    visit(low, 0)
                else:
                    lax.fori_loop(low, high, visit, 0)


def merge(*jobs):
    arrays = [a for job in jobs for a, _, _ in job]
    starts = tuple(tuple((b0, g0) for _, b0, g0 in job) for job in jobs)
    return pl.pallas_call(
        functools.partial(merge_body, starts),
        out_shape=[jax.ShapeDtypeStruct(job[0][0].shape, job[0][0].dtype) for job in jobs],
        name="merge",
    )(*arrays)


def finish_body(parts_ref, out_ref):
    for g in range(out_ref.shape[0]):
        out, _ = merged([(parts_ref[k, g, :HD, :], parts_ref[k, g, HD:, :]) for k in range(parts_ref.shape[0])])
        out_ref[g] = out.T.astype(jnp.bfloat16)


def finish(parts):
    return pl.pallas_call(
        finish_body,
        out_shape=jax.ShapeDtypeStruct((KVH // 2, HD, HD), jnp.bfloat16),
        name="finish",
    )(parts)


def shards(queries, new_kv, prefix_cache, positions, lengths, out_weight):
    devices = lax.axis_size(CTX)
    chips = devices // 2
    ring = chips // HOP
    index = lax.axis_index(CTX)
    chip, core = index // 2, index % 2
    tokens = queries.shape[0]
    per_group = HQ // KVH
    half = HQ * HD // 2

    def take(x, d):
        return lax.ppermute(x, CTX, [(i, (i - 2 * d) % devices) for i in range(devices)])

    def swap(x):
        return lax.ppermute(x, CTX, [(i, i ^ 1) for i in range(devices)])

    def halves(x, axis):
        width = x.shape[axis] // 2
        keep = lax.dynamic_slice_in_dim(x, core * width, width, axis)
        send = lax.dynamic_slice_in_dim(x, (1 - core) * width, width, axis)
        return keep, send

    def in_order(mine, theirs):
        return jnp.where(core == 0, jnp.concatenate([mine, theirs]), jnp.concatenate([theirs, mine]))

    def after(first, *then):
        return lax.optimization_barrier((*then, first))[:-1]

    classes = [[2 * (b + HOP * a) + c for a in range(ring)] for b in range(HOP) for c in range(2)]

    def gathered(block, last=lambda own: ()):
        own = lax.all_gather(block, CTX, axis_index_groups=classes)
        right, left = take(own, 1), take(own, -1)
        done = last(own)
        right, left = after(done, right, left)
        return own, right, left, take(right[: ring // 2], 1), take(left[ring // 2 :], -1), done

    q_mine, q_send = halves(queries, 1)
    n_mine, n_send = halves(new_kv, 1)
    small = swap(jnp.concatenate([q_send, n_send], axis=1))
    theirs = swap(prefix_cache)
    q_block = in_order(q_mine, small[:, :half])
    q_block = q_block.reshape(2 * tokens, KVH // 2, per_group, HD).transpose(1, 0, 2, 3)
    q_block = q_block.reshape(KVH // 2, 2 * tokens * per_group, HD)
    new_rows = jnp.concatenate([n_mine, small[:, half:]])
    new_rows = jnp.pad(new_rows, ((0, TAIL - 2 * tokens), (0, 0))).reshape(TAIL, KVH // 2, 2, HD)
    new_k, new_v = new_rows[:, :, 0].transpose(1, 0, 2), new_rows[:, :, 1].transpose(1, 0, 2)
    pos_of = lambda who: lax.dynamic_slice_in_dim(positions, who * tokens, tokens, 0)
    pos_new = jnp.concatenate([pos_of(index), pos_of(index ^ 1)])
    pos_new = jnp.pad(pos_new, (0, TAIL - 2 * tokens), constant_values=positions.shape[0])[:, None]
    placed = jnp.repeat(positions.reshape(chips, 2 * tokens), per_group, axis=1)
    placed = placed.reshape(ring, HOP, 1, placed.shape[1])
    place = lambda r: lax.dynamic_index_in_dim(placed, (chip + r) % HOP, 1, keepdims=False)
    length_of = lambda who: lax.dynamic_index_in_dim(lengths, who, 0, keepdims=False)
    core_lens = jnp.stack([core, length_of(index), length_of(index ^ 1)]).astype(jnp.int32)
    prepared = prepare(core_lens, prefix_cache, theirs)
    w_mine = lax.dynamic_slice_in_dim(out_weight, core * half, half, 0)

    w_send = lax.dynamic_slice_in_dim(out_weight, (1 - core) * half, half, 0)
    w_theirs = swap(w_send)

    def score(blocks, places):
        return attend(prepared, pos_new, new_k, new_v, blocks, places)

    own, right, left, right_far, left_far, parts_own = gathered(q_block, lambda own: score([own], [place(0)]))
    parts_right = score([right], [place(1)])
    right_far, left_far = after(parts_right, right_far, left_far)
    far = place(2)
    right_far, left_far = score([right_far, left_far], [far[: ring // 2], far[ring // 2 :]])
    parts_left = score([left], [place(-1)])
    parts = [parts_own[0], parts_right[0], parts_left[0]]

    right, left = take(right_far, -1), take(left_far, 1)
    right, left = merge([(parts[1], 0, 0), (right, 0, 0)], [(parts[2], 0, 0), (left, ring // 2, 0)])
    right, left = after(w_theirs, right, left)
    right, left = take(right, -1), take(left, 1)
    (summed,) = merge([(parts[0], 0, 0), (right, 0, 0), (left, 0, 0)])
    own = finish(lax.all_to_all(summed, CTX, 0, 0, axis_index_groups=classes, tiled=True))
    rows = own.reshape(KVH // 2, 2 * tokens, per_group, HD).transpose(1, 0, 2, 3).reshape(2 * tokens, half)

    keep = lax.dynamic_slice_in_dim(rows, core * tokens, tokens, 0)
    other = swap(lax.dynamic_slice_in_dim(rows, (1 - core) * tokens, tokens, 0))
    attended = jnp.where(
        core == 0, jnp.concatenate([keep, other], axis=1), jnp.concatenate([other, keep], axis=1)
    )

    own, right, left, right_far, left_far, _ = gathered(rows)
    mine, other = [], []
    for chunks in ([left, own, right], [right_far, left_far]):
        lhs = jnp.concatenate(chunks).reshape(-1, half)
        other.append(jnp.dot(lhs, w_theirs, preferred_element_type=jnp.float32))
        mine.append(jnp.dot(lhs, w_mine, preferred_element_type=jnp.float32))
    out = jnp.concatenate(mine) + swap(jnp.concatenate(other))
    out = out.astype(jnp.bfloat16).reshape(HOP, ring, 2 * tokens, -1).transpose(1, 0, 2, 3)
    out = lax.dynamic_slice_in_dim(jnp.concatenate([out, out], axis=1), (1 - chip) % HOP, HOP, 1)
    return attended, out.reshape(chips * 2 * tokens, -1)


def solution(mesh):
    return jax.shard_map(
        shards,
        mesh=mesh,
        in_specs=(
            P(SPREAD, None),
            P(SPREAD, None),
            P(SPREAD, None),
            P("groups"),
            P("groups"),
            P(None, CTX),
        ),
        out_specs=(P(SPREAD, None), P("groups", CTX)),
        check_vma=False,
    )
```

```python
import functools
import math

import jax
import jax.numpy as jnp
from jax import lax
from jax.experimental import pallas as pl
from jax.experimental.pallas import tpu as pltpu
from jax.sharding import PartitionSpec as P

HQ = 64
KVH = 4
HD = 128
CTX = "ctx"
SPREAD = ("groups", "ctx")
TILE = 4
HOP = 8
TAIL = 16
ROWS = HD + TAIL
DEAD = -1e30
TO_LOG2 = math.log2(math.e) / math.sqrt(HD)


def prepare_body(lens_ref, mine_k, mine_v, theirs_k, theirs_v, keys_out, values_out):
    slots = mine_k.shape[0]
    lane = lax.broadcasted_iota(jnp.int32, (slots, HD), 1)
    row = lax.broadcasted_iota(jnp.int32, (slots, HD), 0)
    for half, (k_ref, v_ref) in enumerate(((mine_k, mine_v), (theirs_k, theirs_v))):
        dead = jnp.where((lane == 0) & (row >= lens_ref[half + 1]), DEAD, 0.0)
        span = pl.ds(half * slots, slots)
        keys_out[0, span, :HD] = k_ref[...]
        keys_out[0, span, HD:] = dead.astype(jnp.bfloat16)
        values_out[0, :, span] = v_ref[...].T


def prepare(core_lens, cache, theirs):
    slots = cache.shape[0]
    mine = lambda part: pl.BlockSpec((slots, HD), lambda g, s: (0, s[0] * KVH + 2 * g + part))
    return pl.pallas_call(
        prepare_body,
        grid_spec=pltpu.PrefetchScalarGridSpec(
            num_scalar_prefetch=1,
            grid=(KVH // 2,),
            in_specs=[mine(0), mine(1), mine(0), mine(1)],
            out_specs=[
                pl.BlockSpec((1, 2 * slots, 2 * HD), lambda g, s: (g, 0, 0)),
                pl.BlockSpec((1, HD, 2 * slots), lambda g, s: (g, 0, 0)),
            ],
        ),
        out_shape=[
            jax.ShapeDtypeStruct((KVH // 2, 2 * slots, 2 * HD), jnp.bfloat16),
            jax.ShapeDtypeStruct((KVH // 2, HD, 2 * slots), jnp.bfloat16),
        ],
        cost_estimate=pl.CostEstimate(flops=slots * HD * 2048, transcendentals=0, bytes_accessed=10 * slots * HD * KVH),
        name="prepare",
    )(core_lens, cache, cache, theirs, theirs)


def tail_rows(level):
    first = level.astype(jnp.bfloat16).astype(jnp.float32)
    second = (level - first).astype(jnp.bfloat16).astype(jnp.float32)
    third = level - first - second
    row = lax.broadcasted_iota(jnp.int32, (TAIL, level.shape[1]), 0)
    wide = jnp.where(row == 0, first, jnp.where(row == 1, second, jnp.where(row == 2, third, 0.0)))
    return wide.astype(jnp.bfloat16)


def level_of(tail):
    wide = tail.astype(jnp.float32)
    return wide[0:1] + wide[1:2] + wide[2:3]


def attend_body(pos_new, keys_ref, values_ref, new_k, new_v, *refs):
    *refs, all_q, all_pos, all_out = refs
    count = len(refs) // 3
    nt = (((1,), (1,)), ((), ()))
    tn = (((0,), (0,)), ((), ()))

    def softmax(s):
        top = jnp.max(s, axis=0, keepdims=True)
        p = jnp.exp2((s - top) * TO_LOG2)
        return top, jnp.sum(p, axis=0, keepdims=True), p.astype(jnp.bfloat16)

    place = 0
    for q_ref, pos_ref in zip(refs[:count], refs[count : 2 * count]):
        for k in range(q_ref.shape[0]):
            all_q[place + k] = q_ref[k, 0]
            all_pos[place + k] = pos_ref[k]
        place += q_ref.shape[0]

    def tile(i, carry):
        base = i * TILE
        q = jnp.concatenate([all_q[base + k] for k in range(TILE)], axis=0)
        at = jnp.concatenate([all_pos[base + k] for k in range(TILE)], axis=1)
        lane = lax.broadcasted_iota(jnp.int32, q.shape, 1)
        q_wide = jnp.concatenate([q, jnp.where(lane == 0, 1.0, 0.0).astype(q.dtype)], axis=1)
        s = lax.dot_general(keys_ref[0], q_wide, nt, preferred_element_type=jnp.float32)
        top_a, total_a, p = softmax(s)
        out_a = jnp.dot(values_ref[0], p, preferred_element_type=jnp.float32)
        s = lax.dot_general(new_k[0], q, nt, preferred_element_type=jnp.float32)
        top_b, total_b, p = softmax(jnp.where(at >= pos_new[...], s, DEAD))
        out_b = lax.dot_general(new_v[0], p, tn, preferred_element_type=jnp.float32)
        best = jnp.maximum(top_a, top_b)
        keep_a = jnp.exp2((top_a - best) * TO_LOG2)
        keep_b = jnp.exp2((top_b - best) * TO_LOG2)
        total = keep_a * total_a + keep_b * total_b
        out = (keep_a * out_a + keep_b * out_b) * (1.0 / total)
        out = out.astype(jnp.bfloat16)
        tail = tail_rows(best * TO_LOG2 + jnp.log2(total))
        for k in range(TILE):
            lanes = slice(k * HD, (k + 1) * HD)
            all_out[base + k, :HD, :] = out[:, lanes]
            all_out[base + k, HD:, :] = tail[:, lanes]
        return carry

    if place == TILE:
        tile(0, 0)
    else:
        lax.fori_loop(0, place // TILE, tile, 0)
    place = 0
    for out_ref in refs[2 * count :]:
        for k in range(out_ref.shape[0]):
            out_ref[k, 0] = all_out[place + k]
        place += out_ref.shape[0]


def attend(prepared, pos_new, new_k, new_v, blocks, places):
    keys, values = prepared
    per_group = lambda a: pl.BlockSpec((1, *a.shape[1:]), lambda g: (g, 0, 0))
    whole = lambda a: pl.BlockSpec(a.shape, lambda g: (0,) * a.ndim)
    one = lambda a, rows: pl.BlockSpec((a.shape[0], 1, rows, HD), lambda g: (0, g, 0, 0))
    count = sum(b.shape[0] for b in blocks)
    score_count = count * HD * keys.shape[0] * keys.shape[1]
    return pl.pallas_call(
        attend_body,
        grid=(KVH // 2,),
        in_specs=[whole(pos_new), per_group(keys), per_group(values), per_group(new_k), per_group(new_v)]
        + [one(b, HD) for b in blocks]
        + [whole(p) for p in places],
        out_specs=[one(b, ROWS) for b in blocks],
        out_shape=[jax.ShapeDtypeStruct((b.shape[0], KVH // 2, ROWS, HD), jnp.bfloat16) for b in blocks],
        scratch_shapes=[
            pltpu.VMEM((count, HD, HD), jnp.bfloat16),
            pltpu.VMEM((count, 1, HD), jnp.int32),
            pltpu.VMEM((count, ROWS, HD), jnp.bfloat16),
        ],
        compiler_params=pltpu.CompilerParams(vmem_limit_bytes=48 * 1024 * 1024),
        cost_estimate=pl.CostEstimate(
            flops=score_count * 6 * HD,
            transcendentals=score_count,
            bytes_accessed=2 * (keys.size + values.size + 2 * sum(b.size for b in blocks)),
        ),
        name="attend",
    )(pos_new, keys, values, new_k, new_v, *blocks, *places)


def merged(parts):
    levels = [level_of(t) for _, t in parts]
    best = functools.reduce(jnp.maximum, levels)
    weights = [jnp.exp2(v - best) for v in levels]
    total = sum(weights)
    out = sum(w * o.astype(jnp.float32) for w, (o, _) in zip(weights, parts)) * (1.0 / total)
    return out, best + jnp.log2(total)


def merge_body(jobs, *refs):
    ins, outs = list(refs[: -len(jobs)]), refs[-len(jobs) :]
    for starts, out_ref in zip(jobs, outs):
        parts = [(ins.pop(0), b0, g0) for b0, g0 in starts]
        for g in range(out_ref.shape[1]):
            here = [(r, b0, g - g0) for r, b0, g0 in parts if 0 <= g - g0 < r.shape[1]]
            cuts = sorted({c for r, b0, _ in here for c in (b0, b0 + r.shape[0])})
            for low, high in zip(cuts[:-1], cuts[1:]):
                live = [(r, b0, k) for r, b0, k in here if b0 <= low and high <= b0 + r.shape[0]]

                def visit(b, carry, live=live, g=g, out_ref=out_ref):
                    if len(live) == 1:
                        r, b0, k = live[0]
                        out_ref[b, g] = r[b - b0, k]
                        return carry
                    out, level = merged(
                        [(r[b - b0, k, :HD, :], r[b - b0, k, HD:, :]) for r, b0, k in live]
                    )
                    out_ref[b, g, :HD, :] = out.astype(jnp.bfloat16)
                    out_ref[b, g, HD:, :] = tail_rows(level)
                    return carry

                if high - low == 1:
                    visit(low, 0)
                else:
                    lax.fori_loop(low, high, visit, 0)


def merge(*jobs):
    arrays = [a for job in jobs for a, _, _ in job]
    starts = tuple(tuple((b0, g0) for _, b0, g0 in job) for job in jobs)
    return pl.pallas_call(
        functools.partial(merge_body, starts),
        out_shape=[jax.ShapeDtypeStruct(job[0][0].shape, job[0][0].dtype) for job in jobs],
        name="merge",
    )(*arrays)


def finish_body(*refs):
    out_ref = refs[-1]
    for g in range(out_ref.shape[0]):
        out, _ = merged([(r[0, g, :HD, :], r[0, g, HD:, :]) for r in refs[:-1]])
        out_ref[g] = out.T.astype(jnp.bfloat16)


def finish(*arrays):
    return pl.pallas_call(
        finish_body,
        out_shape=jax.ShapeDtypeStruct((KVH // 2, HD, HD), jnp.bfloat16),
        name="finish",
    )(*arrays)


def shards(queries, new_kv, prefix_cache, positions, lengths, out_weight):
    devices = lax.axis_size(CTX)
    chips = devices // 2
    ring = chips // HOP
    reach = HOP // 2
    index = lax.axis_index(CTX)
    chip, core = index // 2, index % 2
    tokens = queries.shape[0]
    per_group = HQ // KVH
    half = HQ * HD // 2

    def take(x, d):
        return lax.ppermute(x, CTX, [(i, (i - 2 * d) % devices) for i in range(devices)])

    def swap(x):
        return lax.ppermute(x, CTX, [(i, i ^ 1) for i in range(devices)])

    def halves(x, axis):
        width = x.shape[axis] // 2
        keep = lax.dynamic_slice_in_dim(x, core * width, width, axis)
        send = lax.dynamic_slice_in_dim(x, (1 - core) * width, width, axis)
        return keep, send

    def in_order(mine, theirs):
        return jnp.where(core == 0, jnp.concatenate([mine, theirs]), jnp.concatenate([theirs, mine]))

    def after(first, *then):
        return lax.optimization_barrier((*then, first))[:-1]

    classes = [[2 * (b + HOP * a) + c for a in range(ring)] for b in range(HOP) for c in range(2)]

    def gathered(block, fill=lambda s, chunks: ()):
        own = lax.all_gather(block, CTX, axis_index_groups=classes)
        chunks = [(own, own)]
        for s in range(1, reach + 1):
            right, left = chunks[-1]
            if s == reach:
                right, left = right[: ring // 2], left[ring // 2 :]
            chunks.append(after(fill(s, chunks), take(right, 1), take(left, -1)))
        return chunks

    q_mine, q_send = halves(queries, 1)
    n_mine, n_send = halves(new_kv, 1)
    small = swap(jnp.concatenate([q_send, n_send], axis=1))
    theirs = swap(prefix_cache)
    q_block = in_order(q_mine, small[:, :half])
    q_block = q_block.reshape(2 * tokens, KVH // 2, per_group, HD).transpose(1, 0, 2, 3)
    q_block = q_block.reshape(KVH // 2, 2 * tokens * per_group, HD)
    new_rows = jnp.concatenate([n_mine, small[:, half:]])
    new_rows = jnp.pad(new_rows, ((0, TAIL - 2 * tokens), (0, 0))).reshape(TAIL, KVH // 2, 2, HD)
    new_k, new_v = new_rows[:, :, 0].transpose(1, 0, 2), new_rows[:, :, 1].transpose(1, 0, 2)
    pos_of = lambda who: lax.dynamic_slice_in_dim(positions, who * tokens, tokens, 0)
    pos_new = jnp.concatenate([pos_of(index), pos_of(index ^ 1)])
    pos_new = jnp.pad(pos_new, (0, TAIL - 2 * tokens), constant_values=positions.shape[0])[:, None]
    placed = jnp.repeat(positions.reshape(chips, 2 * tokens), per_group, axis=1)
    placed = placed.reshape(ring, HOP, 1, placed.shape[1])
    place = lambda r: lax.dynamic_index_in_dim(placed, (chip + r) % HOP, 1, keepdims=False)
    length_of = lambda who: lax.dynamic_index_in_dim(lengths, who, 0, keepdims=False)
    core_lens = jnp.stack([core, length_of(index), length_of(index ^ 1)]).astype(jnp.int32)
    prepared = prepare(core_lens, prefix_cache, theirs)
    w_mine = lax.dynamic_slice_in_dim(out_weight, core * half, half, 0)

    def score(blocks, places):
        return attend(prepared, pos_new, new_k, new_v, blocks, places)

    (weight,) = after(prepared, out_weight)
    w_send = lax.dynamic_slice_in_dim(weight, (1 - core) * half, half, 0)
    parts = {}

    def fill(s, chunks):
        if s == 1:
            return prepared, w_send
        k = s - 2
        if k == 0:
            parts[0] = score([chunks[0][0]], [place(0)])
        else:
            parts[k] = score(list(chunks[k]), [place(k), place(-k)])
        return parts[k]

    chunks = gathered(q_block, fill)
    far = place(reach)
    right, left = score(list(chunks[reach]), [far[: ring // 2], far[ring // 2 :]])
    right, left = take(right, -1), take(left, 1)
    fill(reach + 1, chunks)
    for s in range(reach - 1, 0, -1):
        start = ring // 2 if s == reach - 1 else 0
        right, left = merge([(parts[s][0], 0, 0), (right, 0, 0)], [(parts[s][1], 0, 0), (left, start, 0)])
        right, left = take(right, -1), take(left, 1)
    w_theirs = swap(w_send)
    (summed,) = merge([(parts[0][0], 0, 0), (right, 0, 0), (left, 0, 0)])
    (summed,) = after(w_theirs, summed)
    piece = lambda d: lax.dynamic_slice_in_dim(summed, (chip // HOP + d) % ring, 1, 0)
    own = finish(
        piece(0), take(piece(1), -HOP), take(piece(ring - 1), HOP), take(piece(2), -2 * HOP)
    )
    rows = own.reshape(KVH // 2, 2 * tokens, per_group, HD).transpose(1, 0, 2, 3).reshape(2 * tokens, half)

    keep = lax.dynamic_slice_in_dim(rows, core * tokens, tokens, 0)
    other = swap(lax.dynamic_slice_in_dim(rows, (1 - core) * tokens, tokens, 0))
    attended = jnp.where(
        core == 0, jnp.concatenate([keep, other], axis=1), jnp.concatenate([other, keep], axis=1)
    )

    chunks = gathered(rows)
    near = [c[1] for c in chunks[reach - 1 : 0 : -1]] + [c[0] for c in chunks[:reach]]
    mine, other = [], []
    for group in (near, chunks[reach]):
        lhs = jnp.concatenate(group).reshape(-1, half)
        other.append(jnp.dot(lhs, w_theirs, preferred_element_type=jnp.float32))
        mine.append(jnp.dot(lhs, w_mine, preferred_element_type=jnp.float32))
    out = jnp.concatenate(mine) + swap(jnp.concatenate(other))
    out = out.astype(jnp.bfloat16).reshape(HOP, ring, 2 * tokens, -1).transpose(1, 0, 2, 3)
    out = lax.dynamic_slice_in_dim(jnp.concatenate([out, out], axis=1), (reach - 1 - chip) % HOP, HOP, 1)
    return attended, out.reshape(chips * 2 * tokens, -1)


def solution(mesh):
    return jax.shard_map(
        shards,
        mesh=mesh,
        in_specs=(
            P(SPREAD, None),
            P(SPREAD, None),
            P(SPREAD, None),
            P("groups"),
            P("groups"),
            P(None, CTX),
        ),
        out_specs=(P(SPREAD, None), P("groups", CTX)),
        check_vma=False,
    )
```

```python
import functools
import math

import jax
import jax.numpy as jnp
from jax import lax
from jax.experimental import pallas as pl
from jax.experimental.pallas import tpu as pltpu
from jax.sharding import PartitionSpec as P

HQ = 64
KVH = 4
HD = 128
CTX = "ctx"
SPREAD = ("groups", "ctx")
TILE = 4
HOP = 4
TAIL = 16
ROWS = HD + TAIL
DEAD = -1e30
TO_LOG2 = math.log2(math.e) / math.sqrt(HD)


def prepare_body(lens_ref, mine_k, mine_v, theirs_k, theirs_v, keys_out, values_out):
    slots = mine_k.shape[0]
    lane = lax.broadcasted_iota(jnp.int32, (slots, HD), 1)
    row = lax.broadcasted_iota(jnp.int32, (slots, HD), 0)
    for half, (k_ref, v_ref) in enumerate(((mine_k, mine_v), (theirs_k, theirs_v))):
        dead = jnp.where((lane == 0) & (row >= lens_ref[half + 1]), DEAD, 0.0)
        span = pl.ds(half * slots, slots)
        keys_out[0, span, :HD] = k_ref[...]
        keys_out[0, span, HD:] = dead.astype(jnp.bfloat16)
        values_out[0, :, span] = v_ref[...].T


def prepare(core_lens, cache, theirs):
    slots = cache.shape[0]
    mine = lambda part: pl.BlockSpec((slots, HD), lambda g, s: (0, s[0] * KVH + 2 * g + part))
    return pl.pallas_call(
        prepare_body,
        grid_spec=pltpu.PrefetchScalarGridSpec(
            num_scalar_prefetch=1,
            grid=(KVH // 2,),
            in_specs=[mine(0), mine(1), mine(0), mine(1)],
            out_specs=[
                pl.BlockSpec((1, 2 * slots, 2 * HD), lambda g, s: (g, 0, 0)),
                pl.BlockSpec((1, HD, 2 * slots), lambda g, s: (g, 0, 0)),
            ],
        ),
        out_shape=[
            jax.ShapeDtypeStruct((KVH // 2, 2 * slots, 2 * HD), jnp.bfloat16),
            jax.ShapeDtypeStruct((KVH // 2, HD, 2 * slots), jnp.bfloat16),
        ],
        cost_estimate=pl.CostEstimate(flops=slots * HD * 2048, transcendentals=0, bytes_accessed=10 * slots * HD * KVH),
        name="prepare",
    )(core_lens, cache, cache, theirs, theirs)


def tail_rows(level):
    first = level.astype(jnp.bfloat16).astype(jnp.float32)
    second = (level - first).astype(jnp.bfloat16).astype(jnp.float32)
    third = level - first - second
    row = lax.broadcasted_iota(jnp.int32, (TAIL, level.shape[1]), 0)
    wide = jnp.where(row == 0, first, jnp.where(row == 1, second, jnp.where(row == 2, third, 0.0)))
    return wide.astype(jnp.bfloat16)


def level_of(tail):
    wide = tail.astype(jnp.float32)
    return wide[0:1] + wide[1:2] + wide[2:3]


def attend_body(pos_new, keys_ref, values_ref, new_k, new_v, *refs):
    count = len(refs) // 3
    nt = (((1,), (1,)), ((), ()))
    tn = (((0,), (0,)), ((), ()))

    def softmax(s):
        top = jnp.max(s, axis=0, keepdims=True)
        p = jnp.exp2((s - top) * TO_LOG2)
        return top, jnp.sum(p, axis=0, keepdims=True), p.astype(jnp.bfloat16)

    for q_ref, pos_ref, out_ref in zip(refs[:count], refs[count : 2 * count], refs[2 * count :]):

        def tile(i, carry, q_ref=q_ref, pos_ref=pos_ref, out_ref=out_ref):
            base = i * TILE
            q = jnp.concatenate([q_ref[base + k, 0] for k in range(TILE)], axis=0)
            at = jnp.concatenate([pos_ref[base + k] for k in range(TILE)], axis=1)
            lane = lax.broadcasted_iota(jnp.int32, q.shape, 1)
            q_wide = jnp.concatenate([q, jnp.where(lane == 0, 1.0, 0.0).astype(q.dtype)], axis=1)
            s = lax.dot_general(keys_ref[0], q_wide, nt, preferred_element_type=jnp.float32)
            top_a, total_a, p = softmax(s)
            out_a = jnp.dot(values_ref[0], p, preferred_element_type=jnp.float32)
            s = lax.dot_general(new_k[0], q, nt, preferred_element_type=jnp.float32)
            top_b, total_b, p = softmax(jnp.where(at >= pos_new[...], s, DEAD))
            out_b = lax.dot_general(new_v[0], p, tn, preferred_element_type=jnp.float32)
            best = jnp.maximum(top_a, top_b)
            keep_a = jnp.exp2((top_a - best) * TO_LOG2)
            keep_b = jnp.exp2((top_b - best) * TO_LOG2)
            total = keep_a * total_a + keep_b * total_b
            out = (keep_a * out_a + keep_b * out_b) * (1.0 / total)
            out = out.astype(jnp.bfloat16)
            tail = tail_rows(best * TO_LOG2 + jnp.log2(total))
            for k in range(TILE):
                lanes = slice(k * HD, (k + 1) * HD)
                out_ref[base + k, 0, :HD, :] = out[:, lanes]
                out_ref[base + k, 0, HD:, :] = tail[:, lanes]
            return carry

        if q_ref.shape[0] == TILE:
            tile(0, 0)
        else:
            lax.fori_loop(0, q_ref.shape[0] // TILE, tile, 0)


def attend(prepared, pos_new, new_k, new_v, blocks, places):
    keys, values = prepared
    per_group = lambda a: pl.BlockSpec((1, *a.shape[1:]), lambda g: (g, 0, 0))
    whole = lambda a: pl.BlockSpec(a.shape, lambda g: (0,) * a.ndim)
    one = lambda a, rows: pl.BlockSpec((a.shape[0], 1, rows, HD), lambda g: (0, g, 0, 0))
    score_count = sum(b.shape[0] for b in blocks) * HD * keys.shape[0] * keys.shape[1]
    return pl.pallas_call(
        attend_body,
        grid=(KVH // 2,),
        in_specs=[whole(pos_new), per_group(keys), per_group(values), per_group(new_k), per_group(new_v)]
        + [one(b, HD) for b in blocks]
        + [whole(p) for p in places],
        out_specs=[one(b, ROWS) for b in blocks],
        out_shape=[jax.ShapeDtypeStruct((b.shape[0], KVH // 2, ROWS, HD), jnp.bfloat16) for b in blocks],
        compiler_params=pltpu.CompilerParams(vmem_limit_bytes=48 * 1024 * 1024),
        cost_estimate=pl.CostEstimate(
            flops=score_count * 6 * HD,
            transcendentals=score_count,
            bytes_accessed=2 * (keys.size + values.size + 2 * sum(b.size for b in blocks)),
        ),
        name="attend",
    )(pos_new, keys, values, new_k, new_v, *blocks, *places)


def merged(parts):
    levels = [level_of(t) for _, t in parts]
    best = functools.reduce(jnp.maximum, levels)
    weights = [jnp.exp2(v - best) for v in levels]
    total = sum(weights)
    out = sum(w * o.astype(jnp.float32) for w, (o, _) in zip(weights, parts)) * (1.0 / total)
    return out, best + jnp.log2(total)


def merge_body(jobs, *refs):
    ins, outs = list(refs[: -len(jobs)]), refs[-len(jobs) :]
    for starts, out_ref in zip(jobs, outs):
        parts = [(ins.pop(0), b0, g0) for b0, g0 in starts]
        for g in range(out_ref.shape[1]):
            here = [(r, b0, g - g0) for r, b0, g0 in parts if 0 <= g - g0 < r.shape[1]]
            cuts = sorted({c for r, b0, _ in here for c in (b0, b0 + r.shape[0])})
            for low, high in zip(cuts[:-1], cuts[1:]):
                live = [(r, b0, k) for r, b0, k in here if b0 <= low and high <= b0 + r.shape[0]]

                def visit(b, carry, live=live, g=g, out_ref=out_ref):
                    if len(live) == 1:
                        r, b0, k = live[0]
                        out_ref[b, g] = r[b - b0, k]
                        return carry
                    out, level = merged(
                        [(r[b - b0, k, :HD, :], r[b - b0, k, HD:, :]) for r, b0, k in live]
                    )
                    out_ref[b, g, :HD, :] = out.astype(jnp.bfloat16)
                    out_ref[b, g, HD:, :] = tail_rows(level)
                    return carry

                if high - low == 1:
                    visit(low, 0)
                else:
                    lax.fori_loop(low, high, visit, 0)


def merge(*jobs):
    arrays = [a for job in jobs for a, _, _ in job]
    starts = tuple(tuple((b0, g0) for _, b0, g0 in job) for job in jobs)
    return pl.pallas_call(
        functools.partial(merge_body, starts),
        out_shape=[jax.ShapeDtypeStruct(job[0][0].shape, job[0][0].dtype) for job in jobs],
        name="merge",
    )(*arrays)


def finish_body(*refs):
    out_ref = refs[-1]
    for g in range(out_ref.shape[0]):
        out, _ = merged([(r[0, g, :HD, :], r[0, g, HD:, :]) for r in refs[:-1]])
        out_ref[g] = out.T.astype(jnp.bfloat16)


def finish(*arrays):
    return pl.pallas_call(
        finish_body,
        out_shape=jax.ShapeDtypeStruct((KVH // 2, HD, HD), jnp.bfloat16),
        name="finish",
    )(*arrays)


def shards(queries, new_kv, prefix_cache, positions, lengths, out_weight):
    devices = lax.axis_size(CTX)
    chips = devices // 2
    ring = chips // HOP
    index = lax.axis_index(CTX)
    chip, core = index // 2, index % 2
    tokens = queries.shape[0]
    per_group = HQ // KVH
    half = HQ * HD // 2

    def take(x, d):
        return lax.ppermute(x, CTX, [(i, (i - 2 * d) % devices) for i in range(devices)])

    def swap(x):
        return lax.ppermute(x, CTX, [(i, i ^ 1) for i in range(devices)])

    def halves(x, axis):
        width = x.shape[axis] // 2
        keep = lax.dynamic_slice_in_dim(x, core * width, width, axis)
        send = lax.dynamic_slice_in_dim(x, (1 - core) * width, width, axis)
        return keep, send

    def in_order(mine, theirs):
        return jnp.where(core == 0, jnp.concatenate([mine, theirs]), jnp.concatenate([theirs, mine]))

    def after(first, *then):
        return lax.optimization_barrier((*then, first))[:-1]

    classes = [[2 * (b + HOP * a) + c for a in range(ring)] for b in range(HOP) for c in range(2)]

    def gathered(block, last=lambda own: ()):
        own = lax.all_gather(block, CTX, axis_index_groups=classes)
        right, left = take(own, 1), take(own, -1)
        done = last(own)
        right, left = after(done, right, left)
        return own, right, left, take(right[: ring // 2], 1), take(left[ring // 2 :], -1), done

    q_mine, q_send = halves(queries, 1)
    n_mine, n_send = halves(new_kv, 1)
    small = swap(jnp.concatenate([q_send, n_send], axis=1))
    theirs = swap(prefix_cache)
    q_block = in_order(q_mine, small[:, :half])
    q_block = q_block.reshape(2 * tokens, KVH // 2, per_group, HD).transpose(1, 0, 2, 3)
    q_block = q_block.reshape(KVH // 2, 2 * tokens * per_group, HD)
    new_rows = jnp.concatenate([n_mine, small[:, half:]])
    new_rows = jnp.pad(new_rows, ((0, TAIL - 2 * tokens), (0, 0))).reshape(TAIL, KVH // 2, 2, HD)
    new_k, new_v = new_rows[:, :, 0].transpose(1, 0, 2), new_rows[:, :, 1].transpose(1, 0, 2)
    pos_of = lambda who: lax.dynamic_slice_in_dim(positions, who * tokens, tokens, 0)
    pos_new = jnp.concatenate([pos_of(index), pos_of(index ^ 1)])
    pos_new = jnp.pad(pos_new, (0, TAIL - 2 * tokens), constant_values=positions.shape[0])[:, None]
    placed = jnp.repeat(positions.reshape(chips, 2 * tokens), per_group, axis=1)
    placed = placed.reshape(ring, HOP, 1, placed.shape[1])
    place = lambda r: lax.dynamic_index_in_dim(placed, (chip + r) % HOP, 1, keepdims=False)
    length_of = lambda who: lax.dynamic_index_in_dim(lengths, who, 0, keepdims=False)
    core_lens = jnp.stack([core, length_of(index), length_of(index ^ 1)]).astype(jnp.int32)
    prepared = prepare(core_lens, prefix_cache, theirs)
    w_mine = lax.dynamic_slice_in_dim(out_weight, core * half, half, 0)

    w_send = lax.dynamic_slice_in_dim(out_weight, (1 - core) * half, half, 0)
    w_theirs = swap(w_send)

    def score(blocks, places):
        return attend(prepared, pos_new, new_k, new_v, blocks, places)

    own, right, left, right_far, left_far, parts_own = gathered(q_block, lambda own: score([own], [place(0)]))
    parts_right = score([right], [place(1)])
    right_far, left_far = after(parts_right, right_far, left_far)
    far = place(2)
    right_far, left_far = score([right_far, left_far], [far[: ring // 2], far[ring // 2 :]])
    parts_left = score([left], [place(-1)])
    parts = [parts_own[0], parts_right[0], parts_left[0]]

    right, left = take(right_far, -1), take(left_far, 1)
    right, left = merge([(parts[1], 0, 0), (right, 0, 0)], [(parts[2], 0, 0), (left, ring // 2, 0)])
    right, left = after(w_theirs, right, left)
    right, left = take(right, -1), take(left, 1)
    (summed,) = merge([(parts[0], 0, 0), (right, 0, 0), (left, 0, 0)])
    piece = lambda d: lax.dynamic_slice_in_dim(summed, (chip // HOP + d) % ring, 1, 0)
    high = ring // 2
    up, down = take(piece(high)[:, :1], -HOP), take(piece(high)[:, 1:], HOP)
    for k in range(high - 1, 0, -1):
        start = 1 if k == high - 1 else 0
        up, down = merge([(piece(k), 0, 0), (up, 0, 0)], [(piece(ring - k), 0, 0), (down, 0, start)])
        up, down = take(up, -HOP), take(down, HOP)
    own = finish(piece(0), up, down)
    rows = own.reshape(KVH // 2, 2 * tokens, per_group, HD).transpose(1, 0, 2, 3).reshape(2 * tokens, half)

    keep = lax.dynamic_slice_in_dim(rows, core * tokens, tokens, 0)
    other = swap(lax.dynamic_slice_in_dim(rows, (1 - core) * tokens, tokens, 0))
    attended = jnp.where(
        core == 0, jnp.concatenate([keep, other], axis=1), jnp.concatenate([other, keep], axis=1)
    )

    own, right, left, right_far, left_far, _ = gathered(rows)
    mine, other = [], []
    for chunks in ([left, own, right], [right_far, left_far]):
        lhs = jnp.concatenate(chunks).reshape(-1, half)
        other.append(jnp.dot(lhs, w_theirs, preferred_element_type=jnp.float32))
        mine.append(jnp.dot(lhs, w_mine, preferred_element_type=jnp.float32))
    out = jnp.concatenate(mine) + swap(jnp.concatenate(other))
    out = out.astype(jnp.bfloat16).reshape(HOP, ring, 2 * tokens, -1).transpose(1, 0, 2, 3)
    out = lax.dynamic_slice_in_dim(jnp.concatenate([out, out], axis=1), (1 - chip) % HOP, HOP, 1)
    return attended, out.reshape(chips * 2 * tokens, -1)


def solution(mesh):
    return jax.shard_map(
        shards,
        mesh=mesh,
        in_specs=(
            P(SPREAD, None),
            P(SPREAD, None),
            P(SPREAD, None),
            P("groups"),
            P("groups"),
            P(None, CTX),
        ),
        out_specs=(P(SPREAD, None), P("groups", CTX)),
        check_vma=False,
    )
```
